32 devices in a mesh: groups: 2 (over x), seq: 8 (over z, y), pd: 2 (over core).
Axes of the slice: x: 2, y: 2, z: 4, core: 2. Of those that a mesh axis runs over, the one named last changes fastest.
Arguments:
- streams: bfloat16 [4096, 4, 7168], P(('groups', 'seq'), None, 'pd'), parts along dimension 0, may hold values from -6 to 6
- mix_first: bfloat16 [4, 7168, 24], P(None, 'pd'), may hold values from -0.03125 to 0.03125
- first_layer_bias: float32 [24], replicated, may hold values from -3 to 3
- pre_second: bfloat16 [4, 7168, 4], P(None, 'pd'), may hold values from -0.03125 to 0.03125
- bias_second: float32 [4], replicated, may hold values from -3 to 3
- w_latent: bfloat16 [2, 7168, 576], P(None, ('pd', 'seq')), may hold values from -0.0625 to 0.0625
- latent_gain: float32 [2, 512], replicated, may hold values from 0.5 to 1.5
- out_weight: bfloat16 [512, 7168], P(None, 'pd'), may hold values from -0.25 to 0.25
- span_slot: int32 [32], P('groups'), parts along dimension 0, may hold values from 0 to 15, each once
- block_owner: int32 [16], P('groups'), parts along dimension 0, may hold values from 0 to 7, each once
- prompt_length: int32 [2], P('groups'), parts along dimension 0, may hold values from 1024 to 2048
Outputs:
- cache: bfloat16 [2, 4096, 576], P(None, ('groups', 'seq')), parts along dimension 1
The draws below stay inside these ranges and needn't reach their ends.
There are 2 independent parts, one for each index of `groups`. The reference program is written for one: setup_inputs(seed, part) draws one part's arguments, and reference() takes and returns one part's arrays. A program takes and returns all parts, laid end to end along the dimension named above; an argument that names none is the same for every part. Nothing has to cross between parts.
Inputs may be any that keep to these rules, and one draw needn't show every extreme that they name: span_slot is a permutation; slot q lies in rows q * 128 to q * 128 + 127 of streams. block_owner is a permutation.
All inputs are finite; a program needn't handle non-finite values.
Results may differ from the reference program's by a relative error of at most 0.0058.
Values may be sent and summed in bfloat16 or wider, within the bound.
A program may use at most 128 MiB of HBM per device.

```python
import jax
import jax.numpy as jnp
from jax import lax

D = 7168
LAT = 512
ROPE = 64
KV = 576
RESIDUAL_WAYS = 4
SINK = 20
LAYERS = 2
TOK_DEV = 256
SPAN = 128
TOKENS = 2048
N_SEQ = 8


def block_scale(rng, extent, pieces, low, top_value):
    factor_of, own = 1.0, jax.random.fold_in(rng, 6)
    for dim, shards_of in pieces:
        heights = jnp.exp(jax.random.uniform(jax.random.fold_in(own, dim), (shards_of,), jnp.float32, low / len(pieces), top_value / len(pieces)))
        factor_of = factor_of * jnp.repeat(heights, extent[dim] // shards_of).reshape([-1 if axis == dim else 1 for axis in range(len(extent))])
    return factor_of


def centred(stream_key, extent, deviation, most, pieces=(), kind=jnp.bfloat16):
    factor_of = block_scale(stream_key, extent, pieces, -0.22, 0.18) if pieces else 1.0
    array = jax.random.normal(stream_key, extent, jnp.float32) * deviation * factor_of
    return jnp.minimum(jnp.maximum(array, -most), most).astype(kind)


def setup_inputs(seed: int = 0, part: int = 0) -> dict:
    streams_of = jax.random.split(jax.random.key(seed), 12)
    part_keys = jax.random.split(jax.random.fold_in(streams_of[11], part), 12)
    return {
        "streams": centred(part_keys[0], (TOKENS, RESIDUAL_WAYS, D), 1.0, 6.0, ((0, 8), (2, 2))),
        "mix_first": centred(streams_of[1], (RESIDUAL_WAYS, D, RESIDUAL_WAYS * RESIDUAL_WAYS + 2 * RESIDUAL_WAYS), (RESIDUAL_WAYS * D) ** -0.5, 0.03125, ((1, 2),)),
        "first_layer_bias": centred(streams_of[2], (RESIDUAL_WAYS * RESIDUAL_WAYS + 2 * RESIDUAL_WAYS,), 1.0, 3.0, (), jnp.float32),
        "pre_second": centred(streams_of[3], (RESIDUAL_WAYS, D, RESIDUAL_WAYS), (RESIDUAL_WAYS * D) ** -0.5, 0.03125, ((1, 2),)),
        "bias_second": centred(streams_of[4], (RESIDUAL_WAYS,), 1.0, 3.0, (), jnp.float32),
        "w_latent": centred(streams_of[5], (LAYERS, D, KV), D ** -0.5, 0.0625, ((1, 16),)),
        "latent_gain": jnp.clip(1.0 + 0.1 * jax.random.normal(streams_of[6], (LAYERS, LAT), jnp.float32), 0.5, 1.5),
        "out_weight": centred(streams_of[7], (LAT, D), LAT ** -0.5, 0.25, ((1, 2),)),
        "span_slot": jax.random.permutation(part_keys[8], 2 * N_SEQ).astype(jnp.int32),
        "block_owner": jax.random.permutation(part_keys[9], N_SEQ).astype(jnp.int32),
        "prompt_length": jax.random.randint(part_keys[10], (1,), TOKENS // 2, TOKENS + 1).astype(jnp.int32),
    }


EPSILON = 1e-06
THETA = 10000.0

def doubly_stochastic_normalize(blend_scores_raw):

    def one_sweep(turn_index, matrix):
        matrix = matrix / lax.optimization_barrier(jnp.sum(matrix, axis=2, keepdims=True))
        return matrix / lax.optimization_barrier(jnp.sum(matrix, axis=1, keepdims=True))
    return lax.fori_loop(0, SINK, one_sweep, jnp.exp(blend_scores_raw))

def combine(weights, stream_block):
    weighted = weights[:, 0, None] * stream_block[:, 0, :].astype(jnp.float32)
    for stream_index in range(1, RESIDUAL_WAYS):
        weighted = weighted + weights[:, stream_index, None] * stream_block[:, stream_index, :].astype(jnp.float32)
    return weighted

def coefficients(stream_block, weights, offsets):
    flattened = stream_block.reshape(stream_block.shape[0], -1)
    partial_value = jnp.dot(flattened, weights.reshape(flattened.shape[1], -1), preferred_element_type=jnp.float32)
    square_sum = lax.optimization_barrier(jnp.sum(jnp.square(flattened.astype(jnp.float32)), axis=1))
    rms_scale = jnp.sqrt(square_sum / flattened.shape[1] + EPSILON)
    return partial_value / rms_scale[:, None] + offsets[None, :]

def cache_entry(summed, places, gain_row):
    latent = summed[:, :LAT]
    mean_square = lax.optimization_barrier(jnp.mean(latent * latent, axis=1, keepdims=True))
    normed = latent * lax.rsqrt(mean_square + EPSILON) * gain_row[None, :]
    half_rope = ROPE // 2
    frequency = THETA ** (-jnp.arange(half_rope, dtype=jnp.float32) / half_rope)
    angles = places.astype(jnp.float32)[:, None] * frequency[None, :]
    first_half = summed[:, LAT:LAT + half_rope]
    second = summed[:, LAT + half_rope:]
    cosine_table = jnp.cos(angles)
    sine_values = jnp.sin(angles)
    rotated = jnp.concatenate([first_half * cosine_table - second * sine_values, second * cosine_table + first_half * sine_values], axis=1)
    return jnp.concatenate([normed, rotated], axis=1).astype(jnp.bfloat16)

def reference(streams, mix_first, first_layer_bias, pre_second, bias_second, w_latent, latent_gain, out_weight, span_slot, block_owner, prompt_length):
    total_rows = streams.shape[0]
    slot_span = jnp.zeros((2 * N_SEQ,), jnp.int32).at[span_slot].set(jnp.arange(2 * N_SEQ, dtype=jnp.int32))
    row_ids = jnp.arange(total_rows, dtype=jnp.int32)
    places = slot_span[row_ids // SPAN] * SPAN + row_ids % SPAN

    def one_block(payload):
        stream_block, block_places = payload
        blend_weight = coefficients(stream_block, mix_first, first_layer_bias)
        pre_gate = jax.nn.sigmoid(blend_weight[:, :RESIDUAL_WAYS])
        post_gate = 2.0 * jax.nn.sigmoid(blend_weight[:, RESIDUAL_WAYS:2 * RESIDUAL_WAYS])
        residual_blend_matrix = doubly_stochastic_normalize(blend_weight[:, 2 * RESIDUAL_WAYS:].reshape(-1, RESIDUAL_WAYS, RESIDUAL_WAYS))
        hidden = combine(pre_gate, stream_block).astype(jnp.bfloat16)
        entry_first = cache_entry(jnp.dot(hidden, w_latent[0], preferred_element_type=jnp.float32), block_places, latent_gain[0])
        branch = jnp.dot(entry_first[:, :LAT], out_weight, preferred_element_type=jnp.float32)
        updated = jnp.stack([combine(residual_blend_matrix[:, stream_index, :], stream_block) + post_gate[:, stream_index, None] * branch for stream_index in range(RESIDUAL_WAYS)], axis=1).astype(jnp.bfloat16)
        second_coef = coefficients(updated, pre_second, bias_second)
        hidden_second = combine(jax.nn.sigmoid(second_coef), updated).astype(jnp.bfloat16)
        entry_second = cache_entry(jnp.dot(hidden_second, w_latent[1], preferred_element_type=jnp.float32), block_places, latent_gain[1])
        return jnp.stack([entry_first, entry_second])
    blocks = streams.reshape(N_SEQ, TOK_DEV, RESIDUAL_WAYS, D)
    entries = lax.map(one_block, (blocks, places.reshape(N_SEQ, TOK_DEV)))
    entries = jnp.transpose(entries, (1, 0, 2, 3)).reshape(LAYERS, total_rows, KV)
    in_prompt = places < prompt_length[0]
    entries = jnp.where(in_prompt[None, :, None], entries, jnp.zeros((), jnp.bfloat16))
    row_of_place = jnp.zeros((total_rows,), jnp.int32).at[places].set(row_ids)
    home_segment_per_chip = jnp.zeros((N_SEQ,), jnp.int32).at[block_owner].set(jnp.arange(N_SEQ, dtype=jnp.int32))
    wanted = home_segment_per_chip[row_ids // TOK_DEV] * TOK_DEV + row_ids % TOK_DEV
    return entries[:, row_of_place[wanted], :]
```

```python
import functools

import jax
import jax.numpy as jnp
from jax import lax
from jax.experimental import pallas as pl
from jax.experimental.pallas import tpu as pltpu
from jax.sharding import PartitionSpec as P

LAT = 512
ROPE = 64
RESIDUAL_WAYS = 4
SINK = 20


EPSILON = 1e-06
THETA = 10000.0


MESH = pl.DeviceIdType.MESH
LANES = 128
ROWS = 16
KV = LAT + ROPE
WIDE = LAT + LANES


def ring_position(index, count):
    return jnp.where(index % 2 == 0, index // 2, count - 1 - index // 2)


def ring_index(position, count):
    position = (position + 2 * count) % count
    return jnp.where(position < count // 2, 2 * position, 2 * (count - 1 - position) + 1)


def fused(
    count,
    streams_hbm,
    mix_hbm,
    pre_hbm,
    latent_hbm,
    out_hbm,
    table_ref,
    bias_ref,
    bias_second_ref,
    gain_ref,
    wanted_ref,
    cache_ref,
    held,
    mix,
    pre,
    weight,
    out_weight,
    branch,
    hidden,
    gate_send,
    gate_recv,
    gates,
    down_send,
    down_recv,
    entry,
    masked,
    rows_all,
    final,
    load_sems,
    ring_send,
    ring_recv,
    row_send,
    row_recv,
    pair_send,
    pair_recv,
):
    tokens = held.shape[1]
    width = held.shape[2]
    depth = latent_hbm.shape[1]
    half = tokens // 4
    me = lax.axis_index("seq")
    group = lax.axis_index("groups")
    core = lax.axis_index("pd")
    place = ring_position(me, count)
    following = ring_index(place + 1, count)
    previous = ring_index(place - 1, count)
    twin = group + 1 - 2 * (group % 2)

    to_next = {"seq": following}
    to_prev = {"seq": previous}
    to_twin = {"groups": twin}
    to_pair = {"pd": 1 - core}

    barrier = pltpu.get_barrier_semaphore()
    for target in (to_next, to_prev, to_twin, to_pair):
        pl.semaphore_signal(barrier, inc=1, device_id=target, device_id_type=MESH)
    pl.semaphore_wait(barrier, 4)

    started = []

    def send(src, dst, send_sem, recv_sem, target):
        copy = pltpu.make_async_remote_copy(
            src_ref=src,
            dst_ref=dst,
            send_sem=send_sem,
            recv_sem=recv_sem,
            device_id=target,
            device_id_type=MESH,
        )
        copy.start()
        started.append(copy)

    side = (depth // ROWS // 3) * ROWS
    middle = depth - 2 * side
    side_at = (group % 2) * (side + middle)
    other_at = (1 - group % 2) * (side + middle)

    def part(layer, owner, at, size):
        return weight.at[layer, pl.ds(pl.multiple_of(owner * depth + at, ROWS), size), :]

    def source(layer, step, owner, at, size):
        if step == 0:
            return latent_hbm.at[layer, pl.ds(pl.multiple_of(at, ROWS), size), :]
        return part(layer, owner, at, size)

    def ring_wait(layer, flow, step, dst):
        pltpu.make_async_remote_copy(
            src_ref=dst,
            dst_ref=dst,
            send_sem=ring_send.at[layer, flow, step],
            recv_sem=ring_recv.at[layer, flow, step],
            device_id=to_next,
            device_id_type=MESH,
        ).wait_recv()

    def ring_step(layer, step):
        behind = ring_index(place - step, count)
        ahead = ring_index(place + step, count)
        if step >= 1:
            ring_wait(layer, 0, step - 1, part(layer, behind, side_at, side))
        if step < count - 1:
            send(
                source(layer, step, behind, side_at, side),
                part(layer, behind, side_at, side),
                ring_send.at[layer, 0, step],
                ring_recv.at[layer, 0, step],
                to_next,
            )
        if step >= 1:
            send(
                part(layer, behind, side_at, side),
                part(layer, behind, side_at, side),
                ring_send.at[layer, 2, step - 1],
                ring_recv.at[layer, 2, step - 1],
                to_twin,
            )
            ring_wait(layer, 1, step - 1, part(layer, ahead, side, middle))
        if step < count - 1:
            send(
                source(layer, step, ahead, side, middle),
                part(layer, ahead, side, middle),
                ring_send.at[layer, 1, step],
                ring_recv.at[layer, 1, step],
                to_prev,
            )

    def twin_wait(layer):
        for step in range(count - 1):
            behind = ring_index(place - step - 1, count)
            ring_wait(layer, 2, step, part(layer, behind, other_at, side))

    progress = [0, 0]

    def advance(layer, fraction):
        goal = int(round(fraction * count))
        while progress[layer] < goal:
            ring_step(layer, progress[layer])
            progress[layer] += 1

    ring_step(0, 0)
    progress[0] = 1

    loads = []

    def load(src, dst):
        copy = pltpu.make_async_copy(src, dst, load_sems.at[len(loads)])
        copy.start()
        loads.append(copy)

    for stream in range(RESIDUAL_WAYS):
        load(streams_hbm.at[stream], held.at[stream])
    load(mix_hbm, mix)
    own_rows = pl.ds(pl.multiple_of(me * depth, ROWS), depth)
    load(latent_hbm.at[0], weight.at[0, own_rows, :])
    load(latent_hbm.at[1], weight.at[1, own_rows, :])
    load(out_hbm, out_weight)
    load(pre_hbm, pre)

    def row_block(block):
        return pl.ds(pl.multiple_of(block * ROWS, ROWS), ROWS)

    def exchange_gates(turn, projected, used):
        gate_send[turn, :, 0:used] = projected
        send(
            gate_send.at[turn],
            gate_recv.at[turn],
            pair_send.at[turn],
            pair_recv.at[turn],
            to_pair,
        )

    def gates_total(turn):
        started[-1].wait_recv()
        return (gate_send[turn] + gate_recv[turn]).T

    def scale_of(square_sum):
        return jnp.sqrt(square_sum / (2 * width * RESIDUAL_WAYS) + EPSILON)

    for copy in loads[0:RESIDUAL_WAYS]:
        copy.wait()

    def square_block(block, carry):
        rows = row_block(block)
        total = jnp.zeros((ROWS, width), jnp.float32)
        for stream in range(RESIDUAL_WAYS):
            value = held[stream, rows, :].astype(jnp.float32)
            total = total + value * value
        gate_send[0, rows, :] = jnp.broadcast_to(
            jnp.sum(total, axis=1, keepdims=True), (ROWS, LANES)
        )
        return carry

    lax.fori_loop(0, tokens // ROWS, square_block, 0)
    loads[4].wait()
    advance(0, 0.25)
    projected = jnp.dot(held[0], mix[0], preferred_element_type=jnp.float32)
    for stream in range(1, RESIDUAL_WAYS):
        projected += jnp.dot(held[stream], mix[stream], preferred_element_type=jnp.float32)
    mix_count = mix.shape[2]
    exchange_gates(0, projected, mix_count)
    turned = gates_total(0)
    advance(0, 0.5)
    coef = turned[0:mix_count] / scale_of(turned[mix_count : mix_count + 1]) + bias_ref[...]
    ways = RESIDUAL_WAYS
    gates[...] = jnp.zeros_like(gates)
    gates[0:ways, :] = jax.nn.sigmoid(coef[0:ways])
    gates[ways : 2 * ways, :] = 2.0 * jax.nn.sigmoid(coef[ways : 2 * ways])

    def sweep(turn, matrix):
        matrix = [row / jnp.sum(row, axis=0, keepdims=True) for row in matrix]
        column = matrix[0] + matrix[1] + matrix[2] + matrix[3]
        return [row / column for row in matrix]

    matrix = lax.fori_loop(
        0,
        SINK,
        sweep,
        [jnp.exp(coef[(2 + row) * ways : (3 + row) * ways]) for row in range(ways)],
    )
    for row in range(ways):
        gates[(2 + row) * ways : (3 + row) * ways, :] = matrix[row]
    gate_recv[0] = gates[...].T
    advance(0, 0.625)

    def hidden_block(turn, block, carry):
        rows = row_block(block)
        weights = gate_recv[turn, rows, :]
        total = weights[:, 0:1] * held[0, rows, :].astype(jnp.float32)
        for stream in range(1, RESIDUAL_WAYS):
            total += weights[:, stream : stream + 1] * held[stream, rows, :].astype(
                jnp.float32
            )
        hidden[rows, :] = total.astype(jnp.bfloat16)
        return carry

    lax.fori_loop(0, tokens // ROWS, functools.partial(hidden_block, 0), 0)

    def exchange_down(layer):
        twin_wait(layer)
        loads[5 + layer].wait()
        down_send[layer, :, LAT:] = jnp.zeros((tokens, LANES), jnp.float32)
        down_send[layer, :, 0:KV] = jnp.dot(
            hidden[...], weight[layer], preferred_element_type=jnp.float32
        )
        send(
            down_send.at[layer],
            down_recv.at[layer],
            pair_send.at[2 + layer],
            pair_recv.at[2 + layer],
            to_pair,
        )

    def make_entry(layer, down_copy):
        down_copy.wait_recv()
        total = down_send[layer] + down_recv[layer]
        latent = total[:, 0:LAT]
        square = jnp.mean(latent * latent, axis=1, keepdims=True)
        entry[:, 0:LAT] = (
            latent * lax.rsqrt(square + EPSILON) * gain_ref[layer : layer + 1, :]
        ).astype(jnp.bfloat16)
        key = total[:, LAT:WIDE]
        turned_key = (
            key * table_ref[0]
            + pltpu.roll(key, LANES - ROPE // 2, 1) * table_ref[1]
            + pltpu.roll(key, ROPE // 2, 1) * table_ref[2]
        )
        entry[:, LAT:KV] = turned_key[:, 0:ROPE].astype(jnp.bfloat16)
        keep = table_ref[3][:, 0:1] > 0.5
        masked[...] = jnp.where(keep, entry[...].astype(jnp.float32), 0.0).astype(jnp.bfloat16)
        for span in range(2):
            at = pl.multiple_of(span * (tokens // 2) + core * half, ROWS)
            rows_all[layer, 2 * me + span] = masked[pl.ds(at, half), :]

    def rows_of(layer, owner):
        return rows_all.at[layer, pl.ds(2 * owner, 2)]

    def row_wait(layer, flow, step, dst):
        pltpu.make_async_remote_copy(
            src_ref=dst,
            dst_ref=dst,
            send_sem=row_send.at[layer, flow, step],
            recv_sem=row_recv.at[layer, flow, step],
            device_id=to_next,
            device_id_type=MESH,
        ).wait_recv()

    def row_step(layer, step):
        for flow, sign, hops, target in (
            (0, -1, count // 2, to_next),
            (1, 1, count // 2 - 1, to_prev),
        ):
            block = rows_of(layer, ring_index(place + sign * step, count))
            if 1 <= step <= hops:
                row_wait(layer, flow, step - 1, block)
            if step < hops:
                send(
                    block,
                    block,
                    row_send.at[layer, flow, step],
                    row_recv.at[layer, flow, step],
                    target,
                )

    row_progress = [0, 0]

    def advance_rows(layer, fraction):
        goal = int(round(fraction * (count // 2 + 1)))
        while row_progress[layer] < goal:
            row_step(layer, row_progress[layer])
            row_progress[layer] += 1

    advance(0, 1.0 - 1.0 / count)
    ring_step(1, 0)
    progress[1] = 1
    advance(0, 1.0)
    exchange_down(0)
    down_copy = started[-1]
    advance(1, 0.25)
    make_entry(0, down_copy)
    advance_rows(0, 0.1)
    loads[7].wait()
    piece = width // 7
    for at in range(0, width, piece):
        branch[:, at : at + piece] = jnp.dot(
            entry[:, 0:LAT], out_weight[:, at : at + piece], preferred_element_type=jnp.float32
        )
    advance(1, 0.375)

    def update_block(block, carry):
        rows = row_block(block)
        weights = gate_recv[0, rows, :]
        squares = jnp.zeros((ROWS, 1), jnp.float32)
        step = width // 4
        for at in range(0, width, step):
            columns = slice(at, at + step)
            values = [held[j, rows, columns].astype(jnp.float32) for j in range(ways)]
            added = branch[rows, columns]
            total = jnp.zeros((ROWS, step), jnp.float32)
            for i in range(ways):
                new = weights[:, ways + i : ways + i + 1] * added
                for j in range(ways):
                    k = (2 + i) * ways + j
                    new += weights[:, k : k + 1] * values[j]
                rounded = new.astype(jnp.bfloat16)
                held[i, rows, columns] = rounded
                rounded = rounded.astype(jnp.float32)
                total += rounded * rounded
            squares += jnp.sum(total, axis=1, keepdims=True)
        gate_send[1, rows, :] = jnp.broadcast_to(squares, (ROWS, LANES))
        return carry

    lax.fori_loop(0, tokens // ROWS, update_block, 0)
    loads[8].wait()
    advance(1, 0.5)
    advance_rows(0, 0.4)
    projected = jnp.dot(held[0], pre[0], preferred_element_type=jnp.float32)
    for stream in range(1, RESIDUAL_WAYS):
        projected += jnp.dot(held[stream], pre[stream], preferred_element_type=jnp.float32)
    exchange_gates(1, projected, ways)
    turned = gates_total(1)
    advance(1, 0.625)
    coef = turned[0:ways] / scale_of(turned[ways : ways + 1]) + bias_second_ref[...]
    gates[0:ways, :] = jax.nn.sigmoid(coef)
    gate_recv[1] = gates[...].T
    advance_rows(0, 0.6)
    lax.fori_loop(0, tokens // ROWS, functools.partial(hidden_block, 1), 0)
    advance(1, 0.75)
    advance_rows(0, 0.8)
    advance(1, 0.875)
    advance_rows(0, 1.0)
    advance(1, 1.0)
    exchange_down(1)
    make_entry(1, started[-1])
    advance_rows(1, 1.0)

    for lane in range(2):
        slot = wanted_ref[lane]
        at = pl.multiple_of(lane * (tokens // 2) + core * half, ROWS)
        for layer in range(2):
            final[layer, pl.ds(at, half), :] = rows_all[layer, slot]
    lane_copies = []
    for lane in range(2):
        at = pl.multiple_of(lane * (tokens // 2) + core * half, ROWS)
        block = final.at[:, pl.ds(at, half), :]
        send(block, block, pair_send.at[4 + lane], pair_recv.at[4 + lane], to_pair)
        lane_copies.append(started[-1])
    for copy in lane_copies:
        copy.wait_recv()
    cache_ref[...] = final[...]
    for copy in started:
        copy.wait_send()


def on_device(
    streams,
    mix_first,
    first_layer_bias,
    pre_second,
    bias_second,
    w_latent,
    latent_gain,
    out_weight,
    span_slot,
    block_owner,
    prompt_length,
):
    tokens, ways, width = streams.shape
    span_rows = tokens // 2
    count = lax.axis_size("seq")
    my_index = lax.axis_index("seq")
    own_slots = 2 * my_index + jnp.arange(2, dtype=jnp.int32)
    span_ids = jnp.arange(2 * count, dtype=jnp.int32)
    own_spans = jnp.sum(
        span_ids[None, :] * (span_slot[None, :] == own_slots[:, None]).astype(jnp.int32), axis=1
    )
    places = (
        own_spans[:, None] * span_rows + jnp.arange(span_rows, dtype=jnp.int32)[None, :]
    ).reshape(-1)
    my_block = jnp.sum(
        jnp.arange(count, dtype=jnp.int32) * (block_owner == my_index).astype(jnp.int32)
    )
    wanted = jnp.sum(
        jnp.where(
            span_ids[None, :] == (2 * my_block + jnp.arange(2, dtype=jnp.int32))[:, None],
            span_slot[None, :],
            0,
        ),
        axis=1,
    )
    half_rope = ROPE // 2
    frequency = THETA ** (-jnp.arange(half_rope, dtype=jnp.float32) / half_rope)
    angles = places.astype(jnp.float32)[:, None] * frequency[None, :]
    cosine, sine = jnp.cos(angles), jnp.sin(angles)
    none = jnp.zeros_like(sine)
    keep = (places < prompt_length[0]).astype(jnp.float32)
    table = jnp.stack(
        [
            jnp.concatenate([cosine, cosine, none, none], axis=1),
            jnp.concatenate([-sine, none, none, none], axis=1),
            jnp.concatenate([none, sine, none, none], axis=1),
            jnp.broadcast_to(keep[:, None], (tokens, LANES)),
        ]
    )
    bias_rows = jnp.broadcast_to(first_layer_bias[:, None], (first_layer_bias.shape[0], tokens))
    bias_second_rows = jnp.broadcast_to(bias_second[:, None], (ways, tokens))
    any_space = pl.BlockSpec(memory_space=pl.ANY)
    vmem = pl.BlockSpec(memory_space=pltpu.VMEM)
    steps = count - 1
    return pl.pallas_call(
        functools.partial(fused, count),
        out_shape=jax.ShapeDtypeStruct((2, tokens, KV), jnp.bfloat16),
        in_specs=[any_space] * 5 + [vmem] * 4 + [pl.BlockSpec(memory_space=pltpu.SMEM)],
        out_specs=vmem,
        scratch_shapes=[
            pltpu.VMEM((ways, tokens, width), jnp.bfloat16),
            pltpu.VMEM(mix_first.shape, jnp.bfloat16),
            pltpu.VMEM(pre_second.shape, jnp.bfloat16),
            pltpu.VMEM((2, width, KV), jnp.bfloat16),
            pltpu.VMEM(out_weight.shape, jnp.bfloat16),
            pltpu.VMEM((tokens, width), jnp.float32),
            pltpu.VMEM((tokens, width), jnp.bfloat16),
            pltpu.VMEM((2, tokens, LANES), jnp.float32),
            pltpu.VMEM((2, tokens, LANES), jnp.float32),
            pltpu.VMEM((LANES, tokens), jnp.float32),
            pltpu.VMEM((2, tokens, WIDE), jnp.float32),
            pltpu.VMEM((2, tokens, WIDE), jnp.float32),
            pltpu.VMEM((tokens, KV), jnp.bfloat16),
            pltpu.VMEM((tokens, KV), jnp.bfloat16),
            pltpu.VMEM((2, 2 * count, tokens // 4, KV), jnp.bfloat16),
            pltpu.VMEM((2, tokens, KV), jnp.bfloat16),
            pltpu.SemaphoreType.DMA((9,)),
            pltpu.SemaphoreType.DMA((2, 3, steps)),
            pltpu.SemaphoreType.DMA((2, 3, steps)),
            pltpu.SemaphoreType.DMA((2, 2, count // 2)),
            pltpu.SemaphoreType.DMA((2, 2, count // 2)),
            pltpu.SemaphoreType.DMA((6,)),
            pltpu.SemaphoreType.DMA((6,)),
        ],
        compiler_params=pltpu.CompilerParams(
            collective_id=0, has_side_effects=True, vmem_limit_bytes=62 * 1024 * 1024
        ),
    )(
        jnp.transpose(streams, (1, 0, 2)),
        mix_first,
        pre_second,
        w_latent,
        out_weight,
        table,
        bias_rows,
        bias_second_rows,
        latent_gain,
        wanted,
    )


def solution(mesh):
    placed = (
        P(("groups", "seq"), None, "pd"),
        P(None, "pd", None),
        P(),
        P(None, "pd", None),
        P(),
        P(None, ("pd", "seq"), None),
        P(),
        P(None, "pd"),
        P("groups"),
        P("groups"),
        P("groups"),
    )
    return jax.shard_map(
        on_device,
        mesh=mesh,
        in_specs=placed,
        out_specs=P(None, ("groups", "seq"), None),
        check_vma=False,
    )
```

```python
import functools

import jax
import jax.numpy as jnp
import numpy as np
from jax import lax
from jax.experimental import pallas as pl
from jax.experimental.pallas import tpu as pltpu
from jax.sharding import PartitionSpec as P

LAT = 512
ROPE = 64
RESIDUAL_WAYS = 4
SINK = 20


EPSILON = 1e-06
THETA = 10000.0


MESH = pl.DeviceIdType.MESH
LANES = 128
ROWS = 16
KV = LAT + ROPE
WIDE = LAT + LANES


def ring_position(index, count):
    return jnp.where(index % 2 == 0, index // 2, count - 1 - index // 2)


def ring_index(position, count):
    position = (position + 2 * count) % count
    return jnp.where(position < count // 2, 2 * position, 2 * (count - 1 - position) + 1)


def project(rows, columns):
    return lax.dot_general(
        rows, columns, (((1,), (1,)), ((), ())), preferred_element_type=jnp.float32
    )


def fused(
    count,
    streams_hbm,
    mix_hbm,
    pre_hbm,
    latent_hbm,
    out_hbm,
    turn_ref,
    span_ref,
    bias_ref,
    bias_second_ref,
    gain_ref,
    slots_ref,
    owners_ref,
    length_ref,
    cache_ref,
    table,
    raw,
    spread,
    held,
    mix,
    pre,
    weight,
    out_weight,
    branch,
    hidden,
    gate_send,
    gate_recv,
    gates,
    down_send,
    down_recv,
    entry,
    masked,
    rows_all,
    final,
    load_sems,
    ring_send,
    ring_recv,
    row_send,
    row_recv,
    pair_send,
    pair_recv,
):
    tokens = held.shape[1]
    width = held.shape[2]
    depth = latent_hbm.shape[1]
    half = tokens // 4
    me = lax.axis_index("seq")
    group = lax.axis_index("groups")
    core = lax.axis_index("pd")
    place = ring_position(me, count)
    following = ring_index(place + 1, count)
    previous = ring_index(place - 1, count)
    twin = group + 1 - 2 * (group % 2)

    to_next = {"seq": following}
    to_prev = {"seq": previous}
    to_twin = {"groups": twin}
    to_pair = {"pd": 1 - core}

    barrier = pltpu.get_barrier_semaphore()
    for target in (to_next, to_prev, to_twin, to_pair):
        pl.semaphore_signal(barrier, inc=1, device_id=target, device_id_type=MESH)
    pl.semaphore_wait(barrier, 4)

    started = []

    def send(src, dst, send_sem, recv_sem, target):
        copy = pltpu.make_async_remote_copy(
            src_ref=src,
            dst_ref=dst,
            send_sem=send_sem,
            recv_sem=recv_sem,
            device_id=target,
            device_id_type=MESH,
        )
        copy.start()
        started.append(copy)

    side = (depth // ROWS // 3) * ROWS
    middle = depth - 2 * side
    side_at = (group % 2) * (side + middle)
    other_at = (1 - group % 2) * (side + middle)

    def part(layer, owner, at, size):
        return weight.at[layer, pl.ds(pl.multiple_of(owner * depth + at, ROWS), size), :]

    def source(layer, step, owner, at, size):
        if step == 0:
            return latent_hbm.at[layer, pl.ds(pl.multiple_of(at, ROWS), size), :]
        return part(layer, owner, at, size)

    def ring_wait(layer, flow, step, dst):
        pltpu.make_async_remote_copy(
            src_ref=dst,
            dst_ref=dst,
            send_sem=ring_send.at[layer, flow, step],
            recv_sem=ring_recv.at[layer, flow, step],
            device_id=to_next,
            device_id_type=MESH,
        ).wait_recv()

    def ring_step(layer, step):
        behind = ring_index(place - step, count)
        ahead = ring_index(place + step, count)
        if step >= 1:
            ring_wait(layer, 0, step - 1, part(layer, behind, side_at, side))
        if step < count - 1:
            send(
                source(layer, step, behind, side_at, side),
                part(layer, behind, side_at, side),
                ring_send.at[layer, 0, step],
                ring_recv.at[layer, 0, step],
                to_next,
            )
        if step >= 1:
            send(
                part(layer, behind, side_at, side),
                part(layer, behind, side_at, side),
                ring_send.at[layer, 2, step - 1],
                ring_recv.at[layer, 2, step - 1],
                to_twin,
            )
            ring_wait(layer, 1, step - 1, part(layer, ahead, side, middle))
        if step < count - 1:
            send(
                source(layer, step, ahead, side, middle),
                part(layer, ahead, side, middle),
                ring_send.at[layer, 1, step],
                ring_recv.at[layer, 1, step],
                to_prev,
            )

    def twin_wait(layer):
        for step in range(count - 1):
            behind = ring_index(place - step - 1, count)
            ring_wait(layer, 2, step, part(layer, behind, other_at, side))

    progress = [0, 0]

    def advance(layer, fraction):
        goal = int(round(fraction * count))
        while progress[layer] < goal:
            ring_step(layer, progress[layer])
            progress[layer] += 1

    ring_step(0, 0)
    progress[0] = 1

    loads = []

    def load(src, dst):
        copy = pltpu.make_async_copy(src, dst, load_sems.at[len(loads)])
        copy.start()
        loads.append(copy)

    quarter = tokens // RESIDUAL_WAYS
    for piece in range(RESIDUAL_WAYS):
        part_rows = pl.ds(piece * quarter, quarter)
        load(streams_hbm.at[part_rows], raw.at[part_rows])
    load(mix_hbm, mix)
    own_rows = pl.ds(pl.multiple_of(me * depth, ROWS), depth)
    load(latent_hbm.at[0], weight.at[0, own_rows, :])
    load(latent_hbm.at[1], weight.at[1, own_rows, :])
    load(out_hbm, out_weight)
    load(pre_hbm, pre)

    def row_block(block):
        return pl.ds(pl.multiple_of(block * ROWS, ROWS), ROWS)

    def exchange_gates(turn, projected, used):
        gate_send[turn, :, 0:used] = projected
        send(
            gate_send.at[turn],
            gate_recv.at[turn],
            pair_send.at[turn],
            pair_recv.at[turn],
            to_pair,
        )

    def gates_total(turn, used, offsets):
        copy = started.pop()
        copy.wait()
        total = gate_send[turn] + gate_recv[turn]
        mean = total[:, used : used + 1] / (2 * width * RESIDUAL_WAYS)
        scaled = total / jnp.sqrt(mean + EPSILON)
        scaled = jnp.where(lane < used, scaled, 0.0)
        gate_send[turn, :, :] = scaled
        gate_send[turn, :, 0:used] = scaled[:, 0:used] + offsets
        return gate_send[turn].T

    lane = lax.broadcasted_iota(jnp.int32, (tokens, LANES), 1)
    lane_here = lane[0 : tokens // 2]
    row_here = lax.broadcasted_iota(jnp.int32, (tokens // 2, LANES), 0)
    for span in range(2):
        chosen = jnp.int32(0)
        for candidate in range(2 * count):
            chosen = jnp.where(slots_ref[candidate] == 2 * me + span, candidate, chosen)
        rows = slice(span * (tokens // 2), (span + 1) * (tokens // 2))
        base = span_ref[chosen]
        cosine = base[0:1] * turn_ref[0] - base[1:2] * turn_ref[1]
        sine = base[1:2] * turn_ref[0] + base[0:1] * turn_ref[1]
        table[0, rows, :] = cosine
        table[1, rows, :] = jnp.where(lane_here < ROPE // 2, -sine, 0.0)
        table[2, rows, :] = jnp.where(lane_here < ROPE // 2, 0.0, sine)
        reached = chosen * (tokens // 2) + row_here < length_ref[0]
        table[3, rows, :] = reached.astype(jnp.float32)

    def split_block(block, carry):
        rows = row_block(block)
        total = jnp.zeros((ROWS, LANES), jnp.float32)
        for at in range(0, width, LANES):
            columns = slice(at, at + LANES)
            whole = raw[rows, :, columns].astype(jnp.float32)
            spread[at // LANES] = whole.reshape(ROWS * RESIDUAL_WAYS, LANES)
            for stream in range(RESIDUAL_WAYS):
                value = spread[at // LANES, pl.ds(stream, ROWS, stride=RESIDUAL_WAYS), :]
                held[stream, rows, columns] = value.astype(jnp.bfloat16)
                total = total + value * value
        gate_send[0, rows, :] = jnp.broadcast_to(
            jnp.sum(total, axis=1, keepdims=True), (ROWS, LANES)
        )
        return carry

    for piece in range(RESIDUAL_WAYS):
        loads[piece].wait()
        blocks = quarter // ROWS
        lax.fori_loop(piece * blocks, (piece + 1) * blocks, split_block, 0)
    loads[4].wait()
    advance(0, 0.25)
    projected = project(held[0], mix[0])
    for stream in range(1, RESIDUAL_WAYS):
        projected += project(held[stream], mix[stream])
    mix_count = mix.shape[1]
    exchange_gates(0, projected, mix_count)
    coef = gates_total(0, mix_count, bias_ref[...])
    advance(0, 0.5)
    ways = RESIDUAL_WAYS
    gates[...] = jnp.zeros_like(gates)
    gates[0:ways, :] = jax.nn.sigmoid(coef[0:ways])
    gates[ways : 2 * ways, :] = 2.0 * jax.nn.sigmoid(coef[ways : 2 * ways])

    def sweep(turn, matrix):
        matrix = [row / jnp.sum(row, axis=0, keepdims=True) for row in matrix]
        column = matrix[0] + matrix[1] + matrix[2] + matrix[3]
        return [row / column for row in matrix]

    matrix = lax.fori_loop(
        0,
        SINK,
        sweep,
        [jnp.exp(coef[(2 + row) * ways : (3 + row) * ways]) for row in range(ways)],
    )
    for row in range(ways):
        gates[(2 + row) * ways : (3 + row) * ways, :] = matrix[row]
    gate_recv[0] = gates[...].T
    advance(0, 0.625)

    def hidden_block(turn, block, carry):
        rows = row_block(block)
        weights = gate_recv[turn, rows, :]
        total = weights[:, 0:1] * held[0, rows, :].astype(jnp.float32)
        for stream in range(1, RESIDUAL_WAYS):
            total += weights[:, stream : stream + 1] * held[stream, rows, :].astype(
                jnp.float32
            )
        hidden[rows, :] = total.astype(jnp.bfloat16)
        return carry

    lax.fori_loop(0, tokens // ROWS, functools.partial(hidden_block, 0), 0)

    def exchange_down(layer):
        twin_wait(layer)
        loads[5 + layer].wait()
        down_send[layer, :, LAT:] = jnp.zeros((tokens, LANES), jnp.float32)
        down_send[layer, :, 0:KV] = jnp.dot(
            hidden[...], weight[layer], preferred_element_type=jnp.float32
        )
        send(
            down_send.at[layer],
            down_recv.at[layer],
            pair_send.at[2 + layer],
            pair_recv.at[2 + layer],
            to_pair,
        )

    def make_entry(layer, down_copy):
        down_copy.wait_recv()
        total = down_send[layer] + down_recv[layer]
        latent = total[:, 0:LAT]
        square = jnp.mean(latent * latent, axis=1, keepdims=True)
        entry[:, 0:LAT] = (
            latent * lax.rsqrt(square + EPSILON) * gain_ref[layer : layer + 1, :]
        ).astype(jnp.bfloat16)
        key = total[:, LAT:WIDE]
        turned_key = (
            key * table[0]
            + pltpu.roll(key, LANES - ROPE // 2, 1) * table[1]
            + pltpu.roll(key, ROPE // 2, 1) * table[2]
        )
        entry[:, LAT:KV] = turned_key[:, 0:ROPE].astype(jnp.bfloat16)
        keep = table[3][:, 0:1] > 0.5
        masked[...] = jnp.where(keep, entry[...].astype(jnp.float32), 0.0).astype(jnp.bfloat16)
        for span in range(2):
            at = pl.multiple_of(span * (tokens // 2) + core * half, ROWS)
            rows_all[layer, 2 * me + span] = masked[pl.ds(at, half), :]

    def rows_of(layer, owner):
        return rows_all.at[layer, pl.ds(2 * owner, 2)]

    def row_wait(layer, flow, step, dst):
        pltpu.make_async_remote_copy(
            src_ref=dst,
            dst_ref=dst,
            send_sem=row_send.at[layer, flow, step],
            recv_sem=row_recv.at[layer, flow, step],
            device_id=to_next,
            device_id_type=MESH,
        ).wait_recv()

    def row_step(layer, step):
        for flow, sign, hops, target in (
            (0, -1, count // 2, to_next),
            (1, 1, count // 2 - 1, to_prev),
        ):
            block = rows_of(layer, ring_index(place + sign * step, count))
            if 1 <= step <= hops:
                row_wait(layer, flow, step - 1, block)
            if step < hops:
                send(
                    block,
                    block,
                    row_send.at[layer, flow, step],
                    row_recv.at[layer, flow, step],
                    target,
                )

    row_progress = [0, 0]

    def advance_rows(layer, fraction):
        goal = int(round(fraction * (count // 2 + 1)))
        while row_progress[layer] < goal:
            row_step(layer, row_progress[layer])
            row_progress[layer] += 1

    advance(0, 1.0 - 1.0 / count)
    ring_step(1, 0)
    progress[1] = 1
    advance(0, 1.0)
    exchange_down(0)
    down_copy = started[-1]
    advance(1, 0.25)
    make_entry(0, down_copy)
    advance_rows(0, 0.1)
    loads[7].wait()
    piece = width // 7
    for at in range(0, width, piece):
        branch[:, at : at + piece] = jnp.dot(
            entry[:, 0:LAT], out_weight[:, at : at + piece], preferred_element_type=jnp.float32
        )
    advance(1, 0.375)

    def update_block(block, carry):
        rows = row_block(block)
        weights = gate_recv[0, rows, :]
        squares = jnp.zeros((ROWS, 1), jnp.float32)
        step = width // 4
        for at in range(0, width, step):
            columns = slice(at, at + step)
            values = [held[j, rows, columns].astype(jnp.float32) for j in range(ways)]
            added = branch[rows, columns]
            total = jnp.zeros((ROWS, step), jnp.float32)
            for i in range(ways):
                new = weights[:, ways + i : ways + i + 1] * added
                for j in range(ways):
                    k = (2 + i) * ways + j
                    new += weights[:, k : k + 1] * values[j]
                rounded = new.astype(jnp.bfloat16)
                held[i, rows, columns] = rounded
                rounded = rounded.astype(jnp.float32)
                total += rounded * rounded
            squares += jnp.sum(total, axis=1, keepdims=True)
        gate_send[1, rows, :] = jnp.broadcast_to(squares, (ROWS, LANES))
        return carry

    lax.fori_loop(0, tokens // ROWS, update_block, 0)
    loads[8].wait()
    advance(1, 0.5)
    advance_rows(0, 0.4)
    projected = project(held[0], pre[0])
    for stream in range(1, RESIDUAL_WAYS):
        projected += project(held[stream], pre[stream])
    exchange_gates(1, projected, ways)
    coef = gates_total(1, ways, bias_second_ref[...])
    advance(1, 0.625)
    gates[0:ways, :] = jax.nn.sigmoid(coef[0:ways])
    gate_recv[1] = gates[...].T
    advance_rows(0, 0.6)
    lax.fori_loop(0, tokens // ROWS, functools.partial(hidden_block, 1), 0)
    advance(1, 0.75)
    advance_rows(0, 0.8)
    advance(1, 0.875)
    advance_rows(0, 1.0)
    advance(1, 1.0)
    exchange_down(1)
    make_entry(1, started[-1])
    advance_rows(1, 1.0)

    block_here = jnp.int32(0)
    for block in range(count):
        block_here = jnp.where(owners_ref[block] == me, block, block_here)
    for lane in range(2):
        slot = slots_ref[2 * block_here + lane]
        at = pl.multiple_of(lane * (tokens // 2) + core * half, ROWS)
        for layer in range(2):
            final[layer, pl.ds(at, half), :] = rows_all[layer, slot]
    lane_copies = []
    for lane in range(2):
        at = pl.multiple_of(lane * (tokens // 2) + core * half, ROWS)
        block = final.at[:, pl.ds(at, half), :]
        send(block, block, pair_send.at[4 + lane], pair_recv.at[4 + lane], to_pair)
        lane_copies.append(started[-1])
    for copy in lane_copies:
        copy.wait_recv()
    cache_ref[...] = final[...]
    for copy in started:
        copy.wait_send()


def on_device(
    streams,
    mix_first,
    first_layer_bias,
    pre_second,
    bias_second,
    w_latent,
    latent_gain,
    out_weight,
    span_slot,
    block_owner,
    prompt_length,
):
    tokens, ways, width = streams.shape
    span_rows = tokens // 2
    count = lax.axis_size("seq")
    frequency = THETA ** (-(np.arange(LANES) % (ROPE // 2)) / (ROPE // 2))
    used = np.arange(LANES) < ROPE
    row_angles = np.arange(span_rows)[:, None] * frequency
    span_angles = np.arange(2 * count)[:, None] * span_rows * frequency
    turns = np.stack([np.cos(row_angles) * used, np.sin(row_angles) * used])
    span_turns = np.stack([np.cos(span_angles), np.sin(span_angles)], axis=1)
    any_space = pl.BlockSpec(memory_space=pl.ANY)
    vmem = pl.BlockSpec(memory_space=pltpu.VMEM)
    smem = pl.BlockSpec(memory_space=pltpu.SMEM)
    steps = count - 1
    return pl.pallas_call(
        functools.partial(fused, count),
        out_shape=jax.ShapeDtypeStruct((2, tokens, KV), jnp.bfloat16),
        in_specs=[any_space] * 5 + [vmem] * 5 + [smem] * 3,
        out_specs=vmem,
        scratch_shapes=[
            pltpu.VMEM((4, tokens, LANES), jnp.float32),
            pltpu.VMEM((tokens, ways, width), jnp.bfloat16),
            pltpu.VMEM((width // LANES, ROWS * ways, LANES), jnp.float32),
            pltpu.VMEM((ways, tokens, width), jnp.bfloat16),
            pltpu.VMEM((ways, mix_first.shape[2], width), jnp.bfloat16),
            pltpu.VMEM((ways, pre_second.shape[2], width), jnp.bfloat16),
            pltpu.VMEM((2, width, KV), jnp.bfloat16),
            pltpu.VMEM(out_weight.shape, jnp.bfloat16),
            pltpu.VMEM((tokens, width), jnp.float32),
            pltpu.VMEM((tokens, width), jnp.bfloat16),
            pltpu.VMEM((2, tokens, LANES), jnp.float32),
            pltpu.VMEM((2, tokens, LANES), jnp.float32),
            pltpu.VMEM((LANES, tokens), jnp.float32),
            pltpu.VMEM((2, tokens, WIDE), jnp.float32),
            pltpu.VMEM((2, tokens, WIDE), jnp.float32),
            pltpu.VMEM((tokens, KV), jnp.bfloat16),
            pltpu.VMEM((tokens, KV), jnp.bfloat16),
            pltpu.VMEM((2, 2 * count, tokens // 4, KV), jnp.bfloat16),
            pltpu.VMEM((2, tokens, KV), jnp.bfloat16),
            pltpu.SemaphoreType.DMA((9,)),
            pltpu.SemaphoreType.DMA((2, 3, steps)),
            pltpu.SemaphoreType.DMA((2, 3, steps)),
            pltpu.SemaphoreType.DMA((2, 2, count // 2)),
            pltpu.SemaphoreType.DMA((2, 2, count // 2)),
            pltpu.SemaphoreType.DMA((6,)),
            pltpu.SemaphoreType.DMA((6,)),
        ],
        compiler_params=pltpu.CompilerParams(
            collective_id=0, has_side_effects=True, vmem_limit_bytes=62 * 1024 * 1024
        ),
    )(
        streams,
        jnp.swapaxes(mix_first, 1, 2),
        jnp.swapaxes(pre_second, 1, 2),
        w_latent,
        out_weight,
        turns.astype(np.float32),
        span_turns.astype(np.float32),
        first_layer_bias[None, :],
        bias_second[None, :],
        latent_gain,
        span_slot,
        block_owner,
        prompt_length,
    )


def solution(mesh):
    placed = (
        P(("groups", "seq"), None, "pd"),
        P(None, "pd", None),
        P(),
        P(None, "pd", None),
        P(),
        P(None, ("pd", "seq"), None),
        P(),
        P(None, "pd"),
        P("groups"),
        P("groups"),
        P("groups"),
    )
    return jax.shard_map(
        on_device,
        mesh=mesh,
        in_specs=placed,
        out_specs=P(None, ("groups", "seq"), None),
        check_vma=False,
    )
```
